32 devices in a mesh: dp: 32 (over z, y, x, core), col: 1.
Axes of the slice: x: 2, y: 2, z: 4, core: 2. Of those that a mesh axis runs over, the one named last changes fastest.
Arguments:
- activations: bfloat16 [16384, 16384], P('dp', 'col'), may hold values from -18 to 18
- out_grads: bfloat16 [16384, 53248], P('dp', 'col'), may hold values from -18 to 18
- sketch: bfloat16 [53248, 128], P('col'), may hold values from -6 to 6
Outputs:
- adapter_b: float32 [16384, 64], P(('col', 'dp'))
- adapter_a_t: float32 [53248, 64], P(('col', 'dp'))
The draws below stay inside these ranges and needn't reach their ends.
All inputs are finite; a program needn't handle non-finite values.
Results may differ from the reference program's by a relative error of at most 0.005.
Values may be sent and summed in bfloat16 or wider, within the bound.
No kernel may reach another device: no remote copies, remote signals or barrier semaphores. Data moves between devices by JAX's collectives and lax.ppermute only.
A program may use at most 192 MiB of HBM per device.

```python
import jax
import jax.numpy as jnp
from jax import lax

D = 16384
F = 53248
K = 128
RANK = 64
ITERS = 2
TOK_DEV = 512
TOKENS = 16384


spread_ratio = 30.0


def spiked_field(key, rows, columns, block_rows):
    key_base = jax.random.fold_in(key, 11)
    key_perm = jax.random.fold_in(key, 12)
    values = jax.random.truncated_normal(key_base, -6.0, 6.0, (rows, columns), jnp.float32)
    blocks = rows // block_rows
    pairing = jax.random.permutation(key_perm, blocks)
    row_block = jnp.arange(rows, dtype=jnp.int32) // block_rows
    col_block = jnp.arange(columns, dtype=jnp.int32) // (columns // blocks) % blocks
    chosen = pairing[row_block]
    boost = jnp.where(chosen[:, None] == col_block[None, :], 3.0, 1.0).astype(jnp.float32)
    return values * boost


def drawn_part(key, columns, salt_value):
    key_tokens = jax.random.fold_in(key, 404)
    key_direction = jax.random.fold_in(key, salt_value)
    planted_count = 2 * K
    token_vectors = jax.random.truncated_normal(key_tokens, -3.0, 3.0, (TOKENS, planted_count), jnp.float32)
    directions = jax.random.truncated_normal(key_direction, -3.0, 3.0, (columns, planted_count), jnp.float32)
    position = jnp.arange(planted_count, dtype=jnp.float32)
    amplitude = jnp.exp(-0.5 * jnp.log(jnp.float32(spread_ratio)) * position / K)
    amplitude = amplitude / jnp.sqrt(jnp.sum(amplitude * amplitude))
    return jnp.dot(token_vectors * amplitude[None, :], directions.T, precision=lax.Precision.HIGHEST, preferred_element_type=jnp.float32)


def draw_activations(key, part):
    noisy = spiked_field(jax.random.fold_in(key, 101), TOKENS, D, TOK_DEV)
    total = noisy + drawn_part(key, D, 505)
    return jnp.clip(total, -18.0, 18.0).astype(jnp.bfloat16)


def draw_out_grads(key, part):
    noisy = spiked_field(jax.random.fold_in(key, 202), TOKENS, F, TOK_DEV)
    total = noisy + drawn_part(key, F, 606)
    return jnp.clip(total, -18.0, 18.0).astype(jnp.bfloat16)


def draw_sketch(key, part):
    key_base = jax.random.fold_in(key, 303)
    values = jax.random.truncated_normal(key_base, -6.0, 6.0, (F, K), jnp.float32)
    return values.astype(jnp.bfloat16)


def setup_inputs(seed: int = 0) -> dict:
    arg_keys = jax.random.split(jax.random.key(seed), 4)
    activations = draw_activations(jax.random.fold_in(arg_keys[3], 71), 0)
    out_grads = draw_out_grads(jax.random.fold_in(arg_keys[3], 71), 0)
    sketch = draw_sketch(jax.random.fold_in(arg_keys[3], 71), 0)
    return dict(activations=activations, out_grads=out_grads, sketch=sketch)


def cholesky_basis(panel_in, row_total):
    width = panel_in.shape[1]
    gram_matrix = jnp.dot(panel_in.T.astype(jnp.float32), panel_in.astype(jnp.float32), precision=lax.Precision.HIGHEST, preferred_element_type=jnp.float32)
    identity_k = jnp.eye(width, dtype=jnp.float32)
    shift_value = 1e-05 * jnp.trace(gram_matrix) / width
    lower_factor = jnp.linalg.cholesky(gram_matrix + shift_value * identity_k)
    inverse = jax.scipy.linalg.solve_triangular(lower_factor, identity_k, lower=True)
    scaled = jnp.dot(panel_in.astype(jnp.float32), inverse.T.astype(jnp.float32), precision=lax.Precision.HIGHEST, preferred_element_type=jnp.float32)
    return scaled * jnp.float32(row_total ** 0.5)

def reference(activations, out_grads, sketch):
    right_b = sketch
    left_q = None
    right_p = None
    for iteration in range(ITERS):
        left_s = jnp.dot(out_grads.astype(jnp.float32), right_b.astype(jnp.float32), preferred_element_type=jnp.float32).astype(jnp.bfloat16)
        left_y = lax.dot_general(activations.astype(jnp.float32), left_s.astype(jnp.float32), (((0,), (0,)), ((), ())), preferred_element_type=jnp.float32)
        left_q = cholesky_basis(left_y, D)
        right_t = jnp.dot(activations.astype(jnp.float32), left_q.astype(jnp.bfloat16).astype(jnp.float32), preferred_element_type=jnp.float32).astype(jnp.bfloat16)
        right_z = lax.dot_general(out_grads.astype(jnp.float32), right_t.astype(jnp.float32), (((0,), (0,)), ((), ())), preferred_element_type=jnp.float32)
        right_p = cholesky_basis(right_z, F)
        right_b = right_p.astype(jnp.bfloat16)
    return (left_q[:, :RANK], right_p[:, RANK:])
```

```python
import jax
import jax.numpy as jnp
from jax import lax
from jax.sharding import PartitionSpec as P

D = 16384
F = 53248
RANK = 64
ITERS = 2


def digits_of(count):
    pair = 2 if count % 2 == 0 else 1
    rest = count // pair
    inner = 1
    while inner * inner < rest:
        inner *= 2
    return rest // inner, inner, pair


def swap(value, offset, stride, count):
    return lax.ppermute(value, "dp", [(i, i ^ (offset * stride)) for i in range(count)])


def pick(array, index, axis):
    return lax.dynamic_index_in_dim(array, index, axis, keepdims=False)


def tree_sum(values):
    while len(values) > 1:
        values = [a + b for a, b in zip(values[::2], values[1::2])]
    return values[0]


def scatter_digit(array, axis, me, size, stride, count, wire):
    sent = [pick(array, me ^ k, axis).astype(wire) for k in range(1, size)]
    got = [swap(v, k, stride, count).astype(jnp.float32) for k, v in enumerate(sent, 1)]
    return tree_sum([pick(array, me, axis).astype(jnp.float32)] + got)


def gather_digit(array, axis, me, size, stride, count):
    shape = array.shape[:axis] + (size,) + array.shape[axis:]
    out = jnp.zeros(shape, array.dtype)
    for k in range(size):
        v = array if k == 0 else swap(array, k, stride, count)
        out = lax.dynamic_update_slice_in_dim(out, jnp.expand_dims(v, axis), me ^ k, axis)
    return out


class Ring:
    def __init__(self):
        self.count = lax.axis_size("dp")
        self.no, self.ni, self.np = digits_of(self.count)
        index = lax.axis_index("dp")
        self.pair = index % self.np
        self.inner = (index // self.np) % self.ni
        self.outer = index // (self.np * self.ni)
        self.so = self.np * self.ni
        self.si = self.np

    def scatter(self, partial):
        rows, width = partial.shape
        half = rows // (2 * self.count)
        x = partial.reshape(self.no, self.ni, self.np, 2, half, width)
        x = scatter_digit(x, 2, self.pair, self.np, 1, self.count, jnp.bfloat16)
        a, b = x[:, :, 0], x[:, :, 1]
        a = scatter_digit(a, 1, self.inner, self.ni, self.si, self.count, jnp.bfloat16)
        b = scatter_digit(b, 0, self.outer, self.no, self.so, self.count, jnp.bfloat16)
        a = scatter_digit(a, 0, self.outer, self.no, self.so, self.count, jnp.float32)
        b = scatter_digit(b, 0, self.inner, self.ni, self.si, self.count, jnp.float32)
        return jnp.concatenate([a, b], 0)

    def gather(self, block):
        rows, width = block.shape
        half = rows // 2
        a, b = block[:half], block[half:]
        a = gather_digit(a, 0, self.outer, self.no, self.so, self.count)
        b = gather_digit(b, 0, self.inner, self.ni, self.si, self.count)
        a = gather_digit(a, 1, self.inner, self.ni, self.si, self.count)
        b = gather_digit(b, 0, self.outer, self.no, self.so, self.count)
        x = jnp.stack([a, b], 2)
        x = gather_digit(x, 2, self.pair, self.np, 1, self.count)
        return x.reshape(self.count * rows, width)

    def total(self, value):
        for size, stride in ((self.np, 1), (self.ni, self.si), (self.no, self.so)):
            value = tree_sum([value] + [swap(value, k, stride, self.count) for k in range(1, size)])
        return lax.psum(value, "col")


def cholesky_basis(panel_in, gram_matrix, row_total):
    width = panel_in.shape[1]
    identity_k = jnp.eye(width, dtype=jnp.float32)
    shift_value = 1e-05 * jnp.trace(gram_matrix) / width
    lower_factor = jnp.linalg.cholesky(gram_matrix + shift_value * identity_k)
    inverse = jax.scipy.linalg.solve_triangular(lower_factor, identity_k, lower=True)
    scaled = jnp.dot(
        panel_in, inverse.T, precision=lax.Precision.HIGHEST, preferred_element_type=jnp.float32
    )
    return scaled * jnp.float32(row_total**0.5)


def local_gram(panel_in):
    return jnp.dot(
        panel_in.T, panel_in, precision=lax.Precision.HIGHEST, preferred_element_type=jnp.float32
    )


def body(activations, out_grads, sketch):
    ring = Ring()
    right_b = sketch
    left_rows_q = None
    right_rows_p = None
    for iteration in range(ITERS):
        if iteration:
            right_b = ring.gather(right_rows_p.astype(jnp.bfloat16))
        left_part = jnp.dot(out_grads, right_b, preferred_element_type=jnp.float32)
        left_s = lax.psum(left_part, "col").astype(jnp.bfloat16)
        left_y = ring.scatter(
            lax.dot_general(
                activations, left_s, (((0,), (0,)), ((), ())), preferred_element_type=jnp.float32
            )
        )
        gram_left = ring.total(local_gram(left_y))
        left_rows_q = cholesky_basis(left_y, gram_left, D)
        right_part = jnp.dot(
            activations,
            ring.gather(left_rows_q.astype(jnp.bfloat16)),
            preferred_element_type=jnp.float32,
        )
        right_t = lax.psum(right_part, "col").astype(jnp.bfloat16)
        right_z = ring.scatter(
            lax.dot_general(
                out_grads, right_t, (((0,), (0,)), ((), ())), preferred_element_type=jnp.float32
            )
        )
        gram_right = ring.total(local_gram(right_z))
        right_rows_p = cholesky_basis(right_z, gram_right, F)
    return (left_rows_q[:, :RANK], right_rows_p[:, RANK:])


def solution(mesh):
    return jax.shard_map(
        body,
        mesh=mesh,
        in_specs=(P("dp", "col"), P("dp", "col"), P("col", None)),
        out_specs=(P(("col", "dp"), None), P(("col", "dp"), None)),
        check_vma=False,
    )
```

```python
import jax
import jax.numpy as jnp
from jax import lax
from jax.experimental import pallas as pl
from jax.experimental.pallas import tpu as pltpu
from jax.sharding import PartitionSpec as P

D = 16384
F = 53248
RANK = 64
ITERS = 2
INTERPRET = False


def digits_of(count):
    pair = 2 if count % 2 == 0 else 1
    rest = count // pair
    inner = 1
    while inner * inner < rest:
        inner *= 2
    return rest // inner, inner, pair


def tree_sum(values):
    while len(values) > 1:
        values = [a + b for a, b in zip(values[::2], values[1::2])]
    return values[0]


def panel_kernel(table_ref, coef_ref, matrix_ref, out_ref):
    block = jnp.dot(coef_ref[...], matrix_ref[...], preferred_element_type=jnp.float32)
    out_ref[0] = block.astype(out_ref.dtype)


def panel_blocks(coef_t, matrix, table, rows, dtype):
    width, tokens = coef_t.shape
    blocks = table.shape[0]
    if rows % 128:
        whole = jnp.dot(coef_t, matrix, preferred_element_type=jnp.float32)
        whole = jnp.swapaxes(whole.reshape(width, -1, rows), 0, 1)
        return jnp.take(whole, table, axis=0).astype(dtype)
    return pl.pallas_call(
        panel_kernel,
        grid_spec=pltpu.PrefetchScalarGridSpec(
            num_scalar_prefetch=1,
            grid=(blocks,),
            in_specs=[
                pl.BlockSpec((width, tokens), lambda i, table: (0, 0)),
                pl.BlockSpec((tokens, rows), lambda i, table: (0, table[i])),
            ],
            out_specs=pl.BlockSpec((1, width, rows), lambda i, table: (i, 0, 0)),
        ),
        out_shape=jax.ShapeDtypeStruct((blocks, width, rows), dtype),
        cost_estimate=pl.CostEstimate(
            flops=2 * width * tokens * blocks * rows,
            transcendentals=0,
            bytes_accessed=2 * tokens * blocks * rows,
        ),
        interpret=INTERPRET,
    )(table, coef_t, matrix)


def contract_kernel(table_ref, start_ref, matrix_ref, a_ref, b_ref, out_ref):
    @pl.when(pl.program_id(0) == 0)
    def _():
        out_ref[...] = start_ref[...]

    block = jnp.concatenate([a_ref[0], b_ref[0]], 0)
    out_ref[...] += lax.dot_general(
        matrix_ref[...], block, (((1,), (1,)), ((), ())), preferred_element_type=jnp.float32
    )


def contract_blocks(start, matrix, a, b, table):
    tokens, width = start.shape
    blocks, half, rows = a.shape
    if rows % 128:
        columns = jnp.take(matrix.reshape(tokens, -1, rows), table, axis=1)
        block = jnp.concatenate([a, b], 1)
        return start + lax.dot_general(
            columns, block, (((1, 2), (0, 2)), ((), ())), preferred_element_type=jnp.float32
        )
    return pl.pallas_call(
        contract_kernel,
        grid_spec=pltpu.PrefetchScalarGridSpec(
            num_scalar_prefetch=1,
            grid=(blocks,),
            in_specs=[
                pl.BlockSpec((tokens, width), lambda i, table: (0, 0)),
                pl.BlockSpec((tokens, rows), lambda i, table: (0, table[i])),
                pl.BlockSpec((1, half, rows), lambda i, table: (i, 0, 0)),
                pl.BlockSpec((1, half, rows), lambda i, table: (i, 0, 0)),
            ],
            out_specs=pl.BlockSpec((tokens, width), lambda i, table: (0, 0)),
        ),
        out_shape=jax.ShapeDtypeStruct((tokens, width), jnp.float32),
        cost_estimate=pl.CostEstimate(
            flops=2 * width * tokens * blocks * rows,
            transcendentals=0,
            bytes_accessed=2 * tokens * blocks * rows,
        ),
        interpret=INTERPRET,
    )(table, start, matrix, a, b)


class Digit:
    def __init__(self, size, stride, count, neighbours):
        self.size, self.stride, self.count = size, stride, count
        self.near = neighbours if size == 4 else None

    def swap(self, value, offset):
        pairs = [(i, i ^ (offset * self.stride)) for i in range(self.count)]
        return lax.ppermute(value, "dp", pairs)

    def scatter(self, chunks, wire, relay):
        def move(value, offset):
            return self.swap(value.astype(wire), offset).astype(jnp.float32)

        if not (relay and self.near):
            return tree_sum([chunks[0]] + [move(chunks[k], k) for k in range(1, self.size)])
        n1, n2 = self.near
        far = chunks[n1 ^ n2]
        cut = far.shape[-2] // 2
        top = chunks[n2][..., :cut, :] + move(far[..., :cut, :], n1)
        low = chunks[n1][..., cut:, :] + move(far[..., cut:, :], n2)
        e2 = jnp.concatenate([top, chunks[n2][..., cut:, :]], -2)
        e1 = jnp.concatenate([chunks[n1][..., :cut, :], low], -2)
        return chunks[0] + (move(e1, n1) + move(e2, n2))

    def gather(self, value, relay):
        if not (relay and self.near):
            return [value] + [self.swap(value, k) for k in range(1, self.size)]
        n1, n2 = self.near
        cut = value.shape[-2] // 2
        out = [value] * 4
        out[n1], out[n2] = self.swap(value, n1), self.swap(value, n2)
        top = self.swap(out[n1][..., :cut, :], n2)
        low = self.swap(out[n2][..., cut:, :], n1)
        out[n1 ^ n2] = jnp.concatenate([top, low], -2)
        return out


class Ring:
    def __init__(self):
        count = lax.axis_size("dp")
        no, ni, np_ = digits_of(count)
        index = lax.axis_index("dp")
        self.outer = Digit(no, np_ * ni, count, (1, 3))
        self.inner = Digit(ni, np_, count, (1, 2))
        self.pair = Digit(np_, 1, count, None)
        offsets = (jnp.arange(no)[:, None] * ni + jnp.arange(ni)[None, :]).reshape(-1) * np_
        self.tables = [index ^ (offsets + k).astype(jnp.int32) for k in range(np_)]

    def scatter(self, coef_t, matrix, relay):
        no, ni = self.outer.size, self.inner.size
        width = coef_t.shape[0]
        rows = matrix.shape[1] // self.pair.count
        sent = [panel_blocks(coef_t, matrix, t, rows, jnp.bfloat16) for t in self.tables[1:]]
        got = [self.pair.swap(v, k) for k, v in enumerate(sent, 1)]
        x = panel_blocks(coef_t, matrix, self.tables[0], rows, jnp.float32)
        x = tree_sum([x] + [v.astype(jnp.float32) for v in got])
        x = x.reshape(no, ni, width, rows)
        half = width // 2
        a = self.inner.scatter([x[:, k, :half] for k in range(ni)], jnp.bfloat16, relay)
        b = self.outer.scatter([x[k, :, half:] for k in range(no)], jnp.bfloat16, relay)
        a = self.outer.scatter([a[k] for k in range(no)], jnp.float32, relay)
        b = self.inner.scatter([b[k] for k in range(ni)], jnp.float32, relay)
        return jnp.concatenate([a, b], 0)

    def contract(self, matrix, block, relay):
        no, ni = self.outer.size, self.inner.size
        width, rows = block.shape
        half = width // 2
        a = jnp.stack(self.outer.gather(block[:half], relay), 0)
        b = jnp.stack(self.inner.gather(block[half:], relay), 0)
        a = jnp.stack(self.inner.gather(a, relay), 1).reshape(no * ni, half, rows)
        b = jnp.stack(self.outer.gather(b, relay), 0).reshape(no * ni, half, rows)
        moved = [(self.pair.swap(a, k), self.pair.swap(b, k)) for k in range(1, self.pair.size)]
        out = jnp.zeros((matrix.shape[0], width), jnp.float32)
        for (u, v), table in zip([(a, b)] + moved, self.tables):
            out = contract_blocks(out, matrix, u, v, table)
        return out

    def total(self, value):
        for digit in (self.pair, self.inner, self.outer):
            value = tree_sum([value] + [digit.swap(value, k) for k in range(1, digit.size)])
        return lax.psum(value, "col")


def cholesky_basis(panel_t, gram_matrix, row_total):
    width = panel_t.shape[0]
    identity_k = jnp.eye(width, dtype=jnp.float32)
    shift_value = 1e-05 * jnp.trace(gram_matrix) / width
    lower_factor = jnp.linalg.cholesky(gram_matrix + shift_value * identity_k)
    inverse = jax.scipy.linalg.solve_triangular(lower_factor, identity_k, lower=True)
    scaled = jnp.dot(
        inverse, panel_t, precision=lax.Precision.HIGHEST, preferred_element_type=jnp.float32
    )
    return scaled * jnp.float32(row_total**0.5)


def local_gram(panel_t):
    return lax.dot_general(
        panel_t,
        panel_t,
        (((1,), (1,)), ((), ())),
        precision=lax.Precision.HIGHEST,
        preferred_element_type=jnp.float32,
    )


def body(activations, out_grads, sketch):
    ring = Ring()
    left_part = jnp.dot(out_grads, sketch, preferred_element_type=jnp.float32)
    left_q = None
    right_p = None
    for iteration in range(ITERS):
        if iteration:
            left_part = ring.contract(out_grads, right_p.astype(jnp.bfloat16), True)
        left_s = lax.psum(left_part, "col").astype(jnp.bfloat16)
        left_y = ring.scatter(left_s.T, activations, False)
        left_q = cholesky_basis(left_y, ring.total(local_gram(left_y)), D)
        right_part = ring.contract(activations, left_q.astype(jnp.bfloat16), False)
        right_t = lax.psum(right_part, "col").astype(jnp.bfloat16)
        right_z = ring.scatter(right_t.T, out_grads, True)
        right_p = cholesky_basis(right_z, ring.total(local_gram(right_z)), F)
    return (left_q[:RANK].T, right_p[RANK:].T)


def solution(mesh):
    return jax.shard_map(
        body,
        mesh=mesh,
        in_specs=(P("dp", "col"), P("dp", "col"), P("col", None)),
        out_specs=(P(("col", "dp"), None), P(("col", "dp"), None)),
        check_vma=False,
    )
```

```python
import jax
import jax.numpy as jnp
from jax import lax
from jax.experimental import pallas as pl
from jax.experimental.pallas import tpu as pltpu
from jax.sharding import PartitionSpec as P

D = 16384
F = 53248
RANK = 64
ITERS = 2
INTERPRET = False


def digits_of(count):
    pair = 2 if count % 2 == 0 else 1
    rest = count // pair
    inner = 1
    while inner * inner < rest:
        inner *= 2
    return rest // inner, inner, pair


def tree_sum(values):
    while len(values) > 1:
        values = [a + b for a, b in zip(values[::2], values[1::2])]
    return values[0]


def group_of(blocks, tokens, rows):
    group = 4 if tokens * rows <= 512 * 1024 else 2
    return group if blocks % group == 0 else 1


def column_specs(group, tokens, rows):
    return [
        pl.BlockSpec((tokens, rows), lambda i, table, j=j: (0, table[i * group + j]))
        for j in range(group)
    ]


def panel_kernel(table_ref, coef_ref, *refs):
    out_ref = refs[-1]
    for j, matrix_ref in enumerate(refs[:-1]):
        block = jnp.dot(coef_ref[...], matrix_ref[...], preferred_element_type=jnp.float32)
        out_ref[j] = block.astype(out_ref.dtype)


def panel_blocks(coef_t, matrix, table, rows, dtype):
    width, tokens = coef_t.shape
    blocks = table.shape[0]
    if rows % 128:
        whole = jnp.dot(coef_t, matrix, preferred_element_type=jnp.float32)
        whole = jnp.swapaxes(whole.reshape(width, -1, rows), 0, 1)
        return jnp.take(whole, table, axis=0).astype(dtype)
    group = group_of(blocks, tokens, rows)
    return pl.pallas_call(
        panel_kernel,
        grid_spec=pltpu.PrefetchScalarGridSpec(
            num_scalar_prefetch=1,
            grid=(blocks // group,),
            in_specs=[
                pl.BlockSpec((width, tokens), lambda i, table: (0, 0)),
                *column_specs(group, tokens, rows),
            ],
            out_specs=pl.BlockSpec((group, width, rows), lambda i, table: (i, 0, 0)),
        ),
        out_shape=jax.ShapeDtypeStruct((blocks, width, rows), dtype),
        cost_estimate=pl.CostEstimate(
            flops=2 * width * tokens * blocks * rows,
            transcendentals=0,
            bytes_accessed=2 * tokens * blocks * rows,
        ),
        interpret=INTERPRET,
    )(table, coef_t, *[matrix] * group)


def contract_kernel(table_ref, start_ref, a_ref, b_ref, *refs):
    out_ref = refs[-1]

    @pl.when(pl.program_id(0) == 0)
    def _():
        out_ref[...] = start_ref[...]

    parts = [
        lax.dot_general(
            matrix_ref[...],
            jnp.concatenate([a_ref[j], b_ref[j]], 0),
            (((1,), (1,)), ((), ())),
            preferred_element_type=jnp.float32,
        )
        for j, matrix_ref in enumerate(refs[:-1])
    ]
    out_ref[...] += tree_sum(parts)


def contract_blocks(start, matrix, a, b, table):
    tokens, width = start.shape
    blocks, half, rows = a.shape
    if rows % 128:
        columns = jnp.take(matrix.reshape(tokens, -1, rows), table, axis=1)
        block = jnp.concatenate([a, b], 1)
        return start + lax.dot_general(
            columns, block, (((1, 2), (0, 2)), ((), ())), preferred_element_type=jnp.float32
        )
    group = group_of(blocks, tokens, rows)
    return pl.pallas_call(
        contract_kernel,
        grid_spec=pltpu.PrefetchScalarGridSpec(
            num_scalar_prefetch=1,
            grid=(blocks // group,),
            in_specs=[
                pl.BlockSpec((tokens, width), lambda i, table: (0, 0)),
                pl.BlockSpec((group, half, rows), lambda i, table: (i, 0, 0)),
                pl.BlockSpec((group, half, rows), lambda i, table: (i, 0, 0)),
                *column_specs(group, tokens, rows),
            ],
            out_specs=pl.BlockSpec((tokens, width), lambda i, table: (0, 0)),
        ),
        out_shape=jax.ShapeDtypeStruct((tokens, width), jnp.float32),
        cost_estimate=pl.CostEstimate(
            flops=2 * width * tokens * blocks * rows,
            transcendentals=0,
            bytes_accessed=2 * tokens * blocks * rows,
        ),
        interpret=INTERPRET,
    )(table, start, a, b, *[matrix] * group)


class Digit:
    def __init__(self, size, stride, count, neighbours):
        self.size, self.stride, self.count = size, stride, count
        self.near = neighbours if size == 4 else None

    def swap(self, value, offset):
        pairs = [(i, i ^ (offset * self.stride)) for i in range(self.count)]
        return lax.ppermute(value, "dp", pairs)

    def scatter(self, chunks, wire, relay):
        def move(value, offset):
            return self.swap(value.astype(wire), offset)

        def wide(values):
            return [v.astype(jnp.float32) for v in values]

        if not (relay and self.near):
            got = yield [move(chunks[k], k) for k in range(1, self.size)]
            return tree_sum([chunks[0]] + wide(got))
        n1, n2 = self.near
        far = chunks[n1 ^ n2]
        cut = far.shape[-2] // 2
        top, low = wide((yield [move(far[..., :cut, :], n1), move(far[..., cut:, :], n2)]))
        e2 = jnp.concatenate([chunks[n2][..., :cut, :] + top, chunks[n2][..., cut:, :]], -2)
        e1 = jnp.concatenate([chunks[n1][..., :cut, :], chunks[n1][..., cut:, :] + low], -2)
        u, v = wide((yield [move(e1, n1), move(e2, n2)]))
        return chunks[0] + (u + v)

    def gather(self, value, relay):
        if not (relay and self.near):
            got = yield [self.swap(value, k) for k in range(1, self.size)]
            return [value] + list(got)
        n1, n2 = self.near
        cut = value.shape[-2] // 2
        out = [value] * 4
        out[n1], out[n2] = yield [self.swap(value, n1), self.swap(value, n2)]
        top, low = yield [
            self.swap(out[n1][..., :cut, :], n2),
            self.swap(out[n2][..., cut:, :], n1),
        ]
        out[n1 ^ n2] = jnp.concatenate([top, low], -2)
        return out


def gather_through(first, second, value, relay):
    value = jnp.stack((yield from first.gather(value, relay)), 0)
    return (yield from second.gather(value, relay))


def lockstep(*runs):
    results, answers = [None] * len(runs), [None] * len(runs)
    live = list(range(len(runs)))
    while live:
        asked = {}
        for i in list(live):
            try:
                asked[i] = runs[i].send(answers[i])
            except StopIteration as stop:
                results[i] = stop.value
                live.remove(i)
        if asked:
            asked = lax.optimization_barrier(asked)
            for i in asked:
                answers[i] = asked[i]
    return results


class Ring:
    def __init__(self):
        count = lax.axis_size("dp")
        no, ni, np_ = digits_of(count)
        index = lax.axis_index("dp")
        self.outer = Digit(no, np_ * ni, count, (1, 3))
        self.inner = Digit(ni, np_, count, (1, 2))
        self.pair = Digit(np_, 1, count, None)
        offsets = (jnp.arange(no)[:, None] * ni + jnp.arange(ni)[None, :]).reshape(-1) * np_
        self.tables = [index ^ (offsets + k).astype(jnp.int32) for k in range(np_)]

    def scatter(self, coef_t, matrix, relay):
        no, ni = self.outer.size, self.inner.size
        width = coef_t.shape[0]
        rows = matrix.shape[1] // self.pair.count
        sent = [panel_blocks(coef_t, matrix, t, rows, jnp.bfloat16) for t in self.tables[1:]]
        got = [self.pair.swap(v, k) for k, v in enumerate(sent, 1)]
        x = panel_blocks(coef_t, matrix, self.tables[0], rows, jnp.float32)
        x = tree_sum([x] + [v.astype(jnp.float32) for v in got])
        x = x.reshape(no, ni, width, rows)
        half = width // 2
        a, b = lockstep(
            self.inner.scatter([x[:, k, :half] for k in range(ni)], jnp.bfloat16, relay),
            self.outer.scatter([x[k, :, half:] for k in range(no)], jnp.bfloat16, relay),
        )
        a, b = lockstep(
            self.outer.scatter([a[k] for k in range(no)], jnp.float32, relay),
            self.inner.scatter([b[k] for k in range(ni)], jnp.float32, relay),
        )
        return jnp.concatenate([a, b], 0)

    def contract(self, matrix, block, relay, *beside):
        no, ni = self.outer.size, self.inner.size
        width, rows = block.shape
        half = width // 2
        a, b, *others = lockstep(
            gather_through(self.outer, self.inner, block[:half], relay),
            gather_through(self.inner, self.outer, block[half:], relay),
            *beside,
        )
        a = jnp.stack(a, 1).reshape(no * ni, half, rows)
        b = jnp.stack(b, 0).reshape(no * ni, half, rows)
        moved = [(self.pair.swap(a, k), self.pair.swap(b, k)) for k in range(1, self.pair.size)]
        out = jnp.zeros((matrix.shape[0], width), jnp.float32)
        for (u, v), table in zip([(a, b)] + moved, self.tables):
            out = contract_blocks(out, matrix, u, v, table)
        return out, *others

    def factor(self, panel_t, row_total):
        gram = local_gram(panel_t)
        for digit in (self.pair, self.inner, self.outer):
            got = yield [digit.swap(gram, k) for k in range(1, digit.size)]
            gram = tree_sum([gram] + list(got))
        factor = basis_factor(lax.psum(gram, "col"), row_total)
        return (yield [factor])[0]


def basis_factor(gram_matrix, row_total):
    width = gram_matrix.shape[0]
    identity_k = jnp.eye(width, dtype=jnp.float32)
    shift_value = 1e-05 * jnp.trace(gram_matrix) / width
    lower_factor = jnp.linalg.cholesky(gram_matrix + shift_value * identity_k)
    inverse = jax.scipy.linalg.solve_triangular(lower_factor, identity_k, lower=True)
    return inverse * jnp.float32(row_total**0.5)


def exact_dot(left, right):
    return jnp.dot(
        left, right, precision=lax.Precision.HIGHEST, preferred_element_type=jnp.float32
    )


def local_gram(panel_t):
    return lax.dot_general(
        panel_t,
        panel_t,
        (((1,), (1,)), ((), ())),
        precision=lax.Precision.HIGHEST,
        preferred_element_type=jnp.float32,
    )


def body(activations, out_grads, sketch):
    ring = Ring()
    left_part = jnp.dot(out_grads, sketch, preferred_element_type=jnp.float32)
    left_q = None
    right_p = None
    for iteration in range(ITERS):
        left_s = lax.psum(left_part, "col").astype(jnp.bfloat16)
        left_y = ring.scatter(left_s.T, activations, False)
        factor = ring.factor(left_y, D)
        if iteration:
            right_part, factor = ring.contract(activations, left_y.astype(jnp.bfloat16), False, factor)
            right_part = exact_dot(right_part, factor.T)
            left_q = exact_dot(factor, left_y)
        else:
            left_q = exact_dot(lockstep(factor)[0], left_y)
            (right_part,) = ring.contract(activations, left_q.astype(jnp.bfloat16), False)
        right_t = lax.psum(right_part, "col").astype(jnp.bfloat16)
        right_z = ring.scatter(right_t.T, out_grads, True)
        factor = ring.factor(right_z, F)
        if iteration + 1 < ITERS:
            left_part, factor = ring.contract(out_grads, right_z.astype(jnp.bfloat16), True, factor)
            left_part = exact_dot(left_part, factor.T)
        else:
            right_p = exact_dot(lockstep(factor)[0], right_z)
    return (left_q[:RANK].T, right_p[RANK:].T)


def solution(mesh):
    return jax.shard_map(
        body,
        mesh=mesh,
        in_specs=(P("dp", "col"), P("dp", "col"), P("col", None)),
        out_specs=(P(("col", "dp"), None), P(("col", "dp"), None)),
        check_vma=False,
    )
```
